256 devices in a mesh: shard: 16 (over z, core), width: 4 (over x), shift: 4 (over y).
Axes of the slice: x: 4, y: 4, z: 8, core: 2. Of those that a mesh axis runs over, the one named last changes fastest.
Arguments:
- w_query: float32 [16384, 4096], P(('shift', 'shard'), 'width'), parts along dimension 0, may hold values from -0.125 to 0.125
- first_query: float32 [16384, 4096], P(('shift', 'shard'), 'width'), parts along dimension 0, may hold values from -0.09375 to 0.09375
- second_query: float32 [16384, 4096], P(('shift', 'shard'), 'width'), parts along dimension 0, may hold values from -0.09375 to 0.09375
- w_key: float32 [16384, 1024], P(('shift', 'shard'), 'width'), parts along dimension 0, may hold values from -0.125 to 0.125
- first_key: float32 [16384, 1024], P(('shift', 'shard'), 'width'), parts along dimension 0, may hold values from -0.09375 to 0.09375
- second_key: float32 [16384, 1024], P(('shift', 'shard'), 'width'), parts along dimension 0, may hold values from -0.09375 to 0.09375
- w_value: float32 [16384, 1024], P(('shift', 'shard'), 'width'), parts along dimension 0, may hold values from -0.125 to 0.125
- first_value: float32 [16384, 1024], P(('shift', 'shard'), 'width'), parts along dimension 0, may hold values from -0.09375 to 0.09375
- second_value: float32 [16384, 1024], P(('shift', 'shard'), 'width'), parts along dimension 0, may hold values from -0.09375 to 0.09375
- norm_gain: float32 [16384], P(('shift', 'shard')), parts along dimension 0, may hold values from 0.25 to 1.75
Outputs:
- ready_query: bfloat16 [16384, 4096], P('shift', 'width'), parts along dimension 0
- ready_key: bfloat16 [16384, 1024], P('shift', 'width'), parts along dimension 0
- ready_value: bfloat16 [16384, 1024], P('shift', 'width'), parts along dimension 0
- scale_query: float32 [16384], P(('shift', 'width')), parts along dimension 0
- scale_key: float32 [4096], P(('shift', 'width')), parts along dimension 0
- scale_value: float32 [4096], P(('shift', 'width')), parts along dimension 0
The draws below stay inside these ranges and needn't reach their ends.
There are 4 independent parts, one for each index of `shift`. The reference program is written for one: setup_inputs(seed, part) draws one part's arguments, and reference() takes and returns one part's arrays. A program takes and returns all parts, laid end to end along the dimension named above; each array names one. Nothing has to cross between parts.
All inputs are finite; a program needn't handle non-finite values. Where the reference program divides by a largest or mean magnitude, that divisor is 1e-20 or more.
Results may differ from the reference program's by a relative error of at most 0.001.
Values may be sent and summed in bfloat16 or wider, within the bound.
A program may use at most 128 MiB of HBM per device.

```python
import jax
import jax.numpy as jnp

D_MODEL = 4096
Q_DIM = 4096
KV_DIM = 1024


def spiked(drawn, own_key, source, target, blocks, factor):
    owner, partner = [(jnp.arange(drawn.shape[axis_at]) // (drawn.shape[axis_at] // blocks)).reshape([-1 if axis == axis_at else 1 for axis in range(drawn.ndim)]) for axis_at in (source, target)]
    chosen = jax.random.permutation(own_key, blocks)[partner]
    strong = (owner == chosen) | (owner == (partner + blocks // 2) % blocks)
    return jnp.where(strong, factor * drawn, drawn)


def levels(rng, extent, shards, least, high):
    loudness, own = 1.0, jax.random.fold_in(rng, 6)
    for dim, blocks in shards:
        heights = jnp.exp(jax.random.uniform(jax.random.fold_in(own, dim), (blocks,), jnp.float32, least / len(shards), high / len(shards)))
        loudness = loudness * jnp.repeat(heights, extent[dim] // blocks).reshape([-1 if axis == dim else 1 for axis in range(len(extent))])
    return loudness


def noise(own_key, dims, deviation, limit, split=(), kind=jnp.bfloat16):
    array = deviation * jax.random.normal(own_key, dims, jnp.float32)
    if split:
        array = array * levels(own_key, dims, split, -0.22, 0.18)
    return jnp.clip(array, -limit, limit).astype(kind)


def bell_draw_with(own_key, extent, spread, limit, cuts, heavy, held_as=jnp.bfloat16):
    array = spread * jax.random.normal(own_key, extent, jnp.float32)
    if cuts:
        array = array * levels(own_key, extent, cuts, -0.22, 0.18)
    return jnp.clip(spiked(array, jax.random.fold_in(own_key, 3), *heavy), -limit, limit).astype(held_as)


def setup_inputs(seed: int = 0, part: int = 0) -> dict:
    arg_keys = jax.random.split(jax.random.key(seed), 11)
    part_splits = jax.random.split(jax.random.fold_in(arg_keys[10], part), 11)
    w_query = bell_draw_with(part_splits[0], (D_MODEL, Q_DIM), D_MODEL ** -0.5, 0.125, ((0, 16), (1, 4)), (0, 1, 16, 2.0), jnp.float32)
    first_query = noise(part_splits[1], (D_MODEL, Q_DIM), D_MODEL ** -0.5, 0.09375, ((0, 16), (1, 4)), jnp.float32)
    second_query = noise(part_splits[2], (D_MODEL, Q_DIM), D_MODEL ** -0.5, 0.09375, ((0, 16), (1, 4)), jnp.float32)
    w_key = bell_draw_with(part_splits[3], (D_MODEL, KV_DIM), D_MODEL ** -0.5, 0.125, ((0, 16), (1, 4)), (0, 1, 16, 2.0), jnp.float32)
    first_key = noise(part_splits[4], (D_MODEL, KV_DIM), D_MODEL ** -0.5, 0.09375, ((0, 16), (1, 4)), jnp.float32)
    second_key = noise(part_splits[5], (D_MODEL, KV_DIM), D_MODEL ** -0.5, 0.09375, ((0, 16), (1, 4)), jnp.float32)
    w_value = bell_draw_with(part_splits[6], (D_MODEL, KV_DIM), D_MODEL ** -0.5, 0.125, ((0, 16), (1, 4)), (0, 1, 16, 2.0), jnp.float32)
    first_value = noise(part_splits[7], (D_MODEL, KV_DIM), D_MODEL ** -0.5, 0.09375, ((0, 16), (1, 4)), jnp.float32)
    second_value = noise(part_splits[8], (D_MODEL, KV_DIM), D_MODEL ** -0.5, 0.09375, ((0, 16), (1, 4)), jnp.float32)
    norm_gain = jnp.clip(1.0 + 0.15 * jax.random.normal(part_splits[9], (D_MODEL,), jnp.float32), 0.25, 1.75)
    return dict(w_query=w_query, first_query=first_query, second_query=second_query, w_key=w_key, first_key=first_key, second_key=second_key, w_value=w_value, first_value=first_value, second_value=second_value, norm_gain=norm_gain)


learn_rate = 0.25
hold_rate = 0.8


def reference(w_query, first_query, second_query, w_key, first_key, second_key, w_value, first_value, second_value, norm_gain):
    hold_query = hold_rate * first_query + second_query
    latest_query = w_query - learn_rate * hold_query
    hold_key = hold_rate * first_key + second_key
    latest_key = w_key - learn_rate * hold_key
    hold_value = hold_rate * first_value + second_value
    latest_value = w_value - learn_rate * hold_value
    latest_gained_query = latest_query * norm_gain[:, None]
    latest_gained_key = latest_key * norm_gain[:, None]
    latest_gained_value = latest_value * norm_gain[:, None]
    scale_query = jnp.max(jnp.abs(latest_gained_query), axis=0)
    ready_query = (latest_gained_query / scale_query).astype(jnp.bfloat16)
    scale_key = jnp.max(jnp.abs(latest_gained_key), axis=0)
    ready_key = (latest_gained_key / scale_key).astype(jnp.bfloat16)
    scale_value = jnp.max(jnp.abs(latest_gained_value), axis=0)
    ready_value = (latest_gained_value / scale_value).astype(jnp.bfloat16)
    return ready_query, ready_key, ready_value, scale_query, scale_key, scale_value
```

```python
import jax
import jax.numpy as jnp
from jax import lax
from jax.experimental import pallas as pl
from jax.experimental.pallas import tpu as pltpu
from jax.sharding import PartitionSpec as P

learn_rate = 0.25
hold_rate = 0.8

MESH = pl.DeviceIdType.MESH
AXIS = "shard"
LOADS = 4
STRIP = 16


def make_kernel(n, rows, widths):
    rings = n // 2
    half = rows // 2
    load_rows = rows // LOADS
    starts = [sum(widths[:t]) for t in range(3)]
    total = sum(widths)
    pieces = ((0, 0, half), (0, half, half), (1, 0, rows), (2, 0, rows))
    far = rings // 2

    def kernel(*refs):
        ins = refs[:10]
        gathered, scales = refs[10:13], refs[13:16]
        bufs = refs[16:26]
        fresh, peaks = refs[26:28]
        load_sem, peak_send, peak_recv, ici_send, ici_recv, d2d_send, d2d_recv = refs[28:]

        me = lax.axis_index(AXIS)
        z, core = me // 2, me % 2
        partner = {AXIS: z * 2 + (1 - core)}

        barrier = pltpu.get_barrier_semaphore()
        for off in range(1, n):
            pl.semaphore_signal(
                barrier, inc=1, device_id={AXIS: lax.rem(me + off, n)}, device_id_type=MESH
            )

        def load(a, part):
            span = pl.ds(part * load_rows, load_rows)
            return pltpu.make_async_copy(
                ins[a].at[span, :], bufs[a].at[span, :], load_sem.at[part, a]
            )

        gain_copy = pltpu.make_async_copy(ins[9], bufs[9], load_sem.at[LOADS, 0])
        gain_copy.start()
        for part in range(LOADS):
            for a in range(9):
                load(a, part).start()
        gain_copy.wait()

        tall = jnp.transpose(jnp.broadcast_to(bufs[9][...], (128, rows)))

        tops = [jnp.zeros((8, w), jnp.float32) for w in widths]
        for part in range(LOADS):
            for a in range(9):
                load(a, part).wait()
            for r in range(part * load_rows, (part + 1) * load_rows, 8):
                for t in range(3):
                    w, first, second = (bufs[3 * t + k][r : r + 8, :] for k in range(3))
                    hold = hold_rate * first + second
                    latest = w - learn_rate * hold
                    gain = jnp.concatenate([tall[r : r + 8, :]] * (widths[t] // 128), axis=1)
                    gained = latest * gain
                    fresh[r : r + 8, starts[t] : starts[t] + widths[t]] = gained
                    tops[t] = jnp.maximum(tops[t], jnp.abs(gained))
        for t in range(3):
            peaks[me, :, starts[t] : starts[t] + widths[t]] = jnp.max(tops[t], axis=0, keepdims=True)

        pl.semaphore_wait(barrier, n - 1)

        def tell(off):
            return pltpu.make_async_remote_copy(
                src_ref=peaks.at[me],
                dst_ref=peaks.at[me],
                send_sem=peak_send.at[off],
                recv_sem=peak_recv.at[off],
                device_id={AXIS: lax.rem(me + off, n)},
                device_id_type=MESH,
            )

        def hear(off):
            source = lax.rem(me + n - off, n)
            return pltpu.make_async_remote_copy(
                src_ref=peaks.at[source],
                dst_ref=peaks.at[source],
                send_sem=peak_send.at[off],
                recv_sem=peak_recv.at[off],
                device_id={AXIS: source},
                device_id_type=MESH,
            )

        order = sorted(range(1, n), key=lambda off: -min(off, n - off))
        for off in order:
            tell(off).start()
        for off in range(1, n):
            hear(off).wait_recv()
        top = jnp.max(peaks[...], axis=0)
        for t in range(3):
            scales[t][...] = top[:, starts[t] : starts[t] + widths[t]]

        def at(block, which, p):
            t, first, count = pieces[p]
            return gathered[t].at[pl.ds((block * 2 + which) * rows + first, count), :]

        def ring(step, p, way):
            block = lax.rem(z + rings - step if way == 0 else z + step, rings)
            target = lax.rem(z + 1 if way == 0 else z + rings - 1, rings)
            return pltpu.make_async_remote_copy(
                src_ref=at(block, core, p),
                dst_ref=at(block, core, p),
                send_sem=ici_send.at[way, step, p],
                recv_sem=ici_recv.at[way, step, p],
                device_id={AXIS: target * 2 + core},
                device_id_type=MESH,
            )

        def arrival(step, p, way):
            block = lax.rem(z + rings - 1 - step if way == 0 else z + 1 + step, rings)
            target = lax.rem(z + 1 if way == 0 else z + rings - 1, rings)
            return pltpu.make_async_remote_copy(
                src_ref=at(block, core, p),
                dst_ref=at(block, core, p),
                send_sem=ici_send.at[way, step, p],
                recv_sem=ici_recv.at[way, step, p],
                device_id={AXIS: target * 2 + core},
                device_id_type=MESH,
            )

        def across(block, slot, p, which):
            return pltpu.make_async_remote_copy(
                src_ref=at(block, which, p),
                dst_ref=at(block, which, p),
                send_sem=d2d_send.at[slot, p],
                recv_sem=d2d_recv.at[slot, p],
                device_id=partner,
                device_id_type=MESH,
            )

        def carried(step, p, way):
            return step < far - 1 or p % 2 == way

        sent, crossed = [], []

        def pass_on(step, p, way):
            copy = ring(step, p, way)
            copy.start()
            sent.append(copy)

        def cross(block, slot, p):
            across(block, slot, p, core).start()
            crossed.append((block, slot, p))

        inv = 1.0 / top
        for p, (t, first, count) in enumerate(pieces):
            for r in range(first, first + count, STRIP):
                row = pl.multiple_of(me * rows + r, STRIP)
                value = fresh[r : r + STRIP, starts[t] : starts[t] + widths[t]]
                value = value * inv[:, starts[t] : starts[t] + widths[t]]
                gathered[t][pl.ds(row, STRIP), :] = value.astype(jnp.bfloat16)
        for p in range(4):
            pass_on(0, p, 0)
            pass_on(0, p, 1)
        for p in range(4):
            cross(z, 0, p)

        for step in range(far):
            for p in range(4):
                for way in range(2):
                    if not carried(step, p, way):
                        continue
                    arrival(step, p, way).wait_recv()
                    if step + 1 < far and carried(step + 1, p, way):
                        pass_on(step + 1, p, way)
                    distance = step + 1
                    slot = distance if way == 0 or distance == far else rings - distance
                    block = lax.rem(z + rings - distance if way == 0 else z + distance, rings)
                    cross(block, slot, p)

        for block, slot, p in crossed:
            across(block, slot, p, 1 - core).wait_recv()
        for copy in sent:
            copy.wait_send()
        for block, slot, p in crossed:
            across(block, slot, p, core).wait_send()
        for off in range(1, n):
            tell(off).wait_send()

    out_shape = tuple(pltpu.VMEM((n * rows, w), jnp.bfloat16) for w in widths) + tuple(
        pltpu.VMEM((1, w), jnp.float32) for w in widths
    )
    vmem = pl.BlockSpec(memory_space=pltpu.VMEM)
    return pl.pallas_call(
        kernel,
        name="update_gather",
        out_shape=out_shape,
        in_specs=[pl.BlockSpec(memory_space=pltpu.HBM)] * 10,
        out_specs=(vmem,) * 6,
        scratch_shapes=[pltpu.VMEM((rows, w), jnp.float32) for w in widths for _ in range(3)]
        + [
            pltpu.VMEM((1, rows), jnp.float32),
            pltpu.VMEM((rows, total), jnp.float32),
            pltpu.VMEM((n, 1, total), jnp.float32),
            pltpu.SemaphoreType.DMA((LOADS + 1, 9)),
            pltpu.SemaphoreType.DMA((n,)),
            pltpu.SemaphoreType.DMA((n,)),
            pltpu.SemaphoreType.DMA((2, far, 4)),
            pltpu.SemaphoreType.DMA((2, far, 4)),
            pltpu.SemaphoreType.DMA((rings, 4)),
            pltpu.SemaphoreType.DMA((rings, 4)),
        ],
        compiler_params=pltpu.CompilerParams(
            collective_id=0, has_side_effects=True, vmem_limit_bytes=40 * 1024 * 1024
        ),
    )


def body(
    w_query,
    first_query,
    second_query,
    w_key,
    first_key,
    second_key,
    w_value,
    first_value,
    second_value,
    norm_gain,
):
    n = lax.axis_size(AXIS)
    rows = w_query.shape[0]
    widths = (w_query.shape[1], w_key.shape[1], w_value.shape[1])
    call = make_kernel(n, rows, widths)
    large = (
        w_query,
        first_query,
        second_query,
        w_key,
        first_key,
        second_key,
        w_value,
        first_value,
        second_value,
        norm_gain.reshape(1, rows),
    )
    large = [pltpu.with_memory_space_constraint(a, pltpu.HBM) for a in large]
    outs = call(*large)
    return tuple(outs[:3]) + tuple(s.reshape(-1) for s in outs[3:])


def solution(mesh):
    by_row = P(("shift", "shard"), "width")
    in_specs = (by_row,) * 9 + (P(("shift", "shard")),)
    out_specs = (P("shift", "width"),) * 3 + (P(("shift", "width")),) * 3
    return jax.shard_map(body, mesh=mesh, in_specs=in_specs, out_specs=out_specs, check_vma=False)
```

```python
import jax
import jax.numpy as jnp
from jax import lax
from jax.experimental import pallas as pl
from jax.experimental.pallas import tpu as pltpu
from jax.sharding import PartitionSpec as P

learn_rate = 0.25
hold_rate = 0.8

MESH = pl.DeviceIdType.MESH
AXIS = "shard"
LOADS = 4
STRIP = 16
EARLY = 32
CUT = 64
FAR_CUTS = ((64, 48, 16), (64, 48, 16))


def make_kernel(n, rows, widths):
    rings = n // 2
    far = rings // 2
    load_rows = rows // LOADS
    starts = [sum(widths[:t]) for t in range(3)]
    total = sum(widths)
    whole = tuple((first, CUT) for first in range(0, rows, CUT))
    assert sum(map(sum, FAR_CUTS)) == rows

    def last_pieces(way):
        first, out = way * sum(FAR_CUTS[0]), []
        for count in FAR_CUTS[way]:
            out.append((first, count))
            first += count
        return tuple(out)

    def carried(step, way):
        if step == far - 1:
            return last_pieces(way)
        if step == 0 and EARLY:
            return ((EARLY, CUT - EARLY),) + whole[1:]
        return whole

    slots, slot_of = 0, {}
    for way in range(2):
        for step in range(far):
            for p in range(len(carried(step, way))):
                slot_of[way, step, p] = slots
                slots += 1

    def kernel(*refs):
        ins = refs[:10]
        gathered, scales = refs[10], refs[11:14]
        land, gains, fresh, peaks, early = refs[14:19]
        load_sem, one_sem, ici_recv = refs[19:]
        gain_sem, peak_send, peak_recv, ici_send, d2d_send, d2d_recv, early_send = (
            one_sem.at[i] for i in range(7)
        )

        me = lax.axis_index(AXIS)
        z, core = me // 2, me % 2
        partner = {AXIS: z * 2 + (1 - core)}
        ahead = (lax.rem(z + 1, rings), lax.rem(z + rings - 1, rings))

        barrier = pltpu.get_barrier_semaphore()
        for off in range(1, n):
            pl.semaphore_signal(
                barrier, inc=1, device_id={AXIS: lax.rem(me + off, n)}, device_id_type=MESH
            )

        gain_copy = pltpu.make_async_copy(ins[9], gains, gain_sem)
        gain_copy.start()
        place, at = [], 0
        for t in range(3):
            for _ in range(3):
                place.append((at, widths[t]))
                at += widths[t]
        for part in range(LOADS):
            span = pl.ds(part * load_rows, load_rows)
            for a, (first, width) in enumerate(place):
                pltpu.make_async_copy(
                    ins[a].at[span, :],
                    land.at[span, pl.ds(first, width)],
                    load_sem.at[part],
                ).start()

        gain_copy.wait()
        tall = jnp.transpose(jnp.broadcast_to(gains[...], (128, rows)))
        tops = [jnp.zeros((8, w), jnp.float32) for w in widths]
        for part in range(LOADS):
            span = pl.ds(part * load_rows, load_rows)
            pltpu.make_async_copy(land.at[span, :], land.at[span, :], load_sem.at[part]).wait()
            for r in range(part * load_rows, (part + 1) * load_rows, 8):
                for t in range(3):
                    w, first, second = (
                        land[r : r + 8, place[3 * t + k][0] : place[3 * t + k][0] + widths[t]]
                        for k in range(3)
                    )
                    hold = hold_rate * first + second
                    latest = w - learn_rate * hold
                    gain = jnp.concatenate([tall[r : r + 8, :]] * (widths[t] // 128), axis=1)
                    gained = latest * gain
                    fresh[r : r + 8, starts[t] : starts[t] + widths[t]] = gained
                    tops[t] = jnp.maximum(tops[t], jnp.abs(gained))
        for t in range(3):
            peaks[me, :, starts[t] : starts[t] + widths[t]] = jnp.max(tops[t], axis=0, keepdims=True)

        pl.semaphore_wait(barrier, n - 1)

        for off in sorted(range(1, n), key=lambda off: -min(off, n - off)):
            pltpu.make_async_remote_copy(
                src_ref=peaks.at[me],
                dst_ref=peaks.at[me],
                send_sem=peak_send,
                recv_sem=peak_recv,
                device_id={AXIS: lax.rem(me + off, n)},
                device_id_type=MESH,
            ).start()

        def early_copy(way):
            return pltpu.make_async_remote_copy(
                src_ref=fresh.at[pl.ds(0, EARLY), :],
                dst_ref=early.at[way],
                send_sem=early_send,
                recv_sem=one_sem.at[7 + way],
                device_id={AXIS: ahead[way] * 2 + core},
                device_id_type=MESH,
            )

        if EARLY:
            for way in range(2):
                early_copy(way).start()

        others = peaks.at[pl.ds(0, n - 1)]
        pltpu.make_async_copy(others, others, peak_recv).wait()
        top = jnp.max(peaks[...], axis=0)
        inv = 1.0 / top

        def block_at(distance, way):
            if distance == 0:
                return z
            return lax.rem(z + rings - distance if way == 0 else z + distance, rings)

        def rows_of(block, first, count):
            return gathered.at[pl.ds(me_rows(block) + first, count), :]

        def me_rows(block):
            return pl.multiple_of((block * 2 + core) * rows, STRIP)

        def hop(block, way, step, p):
            first, count = carried(step, way)[p]
            return pltpu.make_async_remote_copy(
                src_ref=rows_of(block, first, count),
                dst_ref=rows_of(block, first, count),
                send_sem=ici_send,
                recv_sem=ici_recv.at[slot_of[way, step, p]],
                device_id={AXIS: ahead[way] * 2 + core},
                device_id_type=MESH,
            )

        def cross(block, first, count):
            pltpu.make_async_remote_copy(
                src_ref=rows_of(block, first, count),
                dst_ref=rows_of(block, first, count),
                send_sem=d2d_send,
                recv_sem=d2d_recv,
                device_id=partner,
                device_id_type=MESH,
            ).start()

        def settle(source, base, first, count):
            for r in range(0, count, STRIP):
                row = pl.multiple_of(base + first + r, STRIP)
                gathered[pl.ds(row, STRIP), :] = (source(r) * inv).astype(jnp.bfloat16)

        if EARLY:
            settle(lambda r: fresh[r : r + STRIP, :], me_rows(z), 0, EARLY)
        settle(lambda r: fresh[EARLY + r : EARLY + r + STRIP, :], me_rows(z), EARLY, rows - EARLY)
        for p in range(len(whole)):
            for way in range(2):
                hop(z, way, 0, p).start()
        for first, count in whole:
            cross(z, first, count)
        for t in range(3):
            scales[t][...] = top[:, starts[t] : starts[t] + widths[t]]

        if EARLY:
            for way in range(2):
                early_copy(way).wait_recv()
                settle(lambda r: early[way, r : r + STRIP, :], me_rows(block_at(1, way)), 0, EARLY)

        for step in range(far):
            for p in range(max(len(carried(step, way)) for way in range(2))):
                for way in range(2):
                    if p >= len(carried(step, way)):
                        continue
                    block = block_at(step + 1, way)
                    hop(block, way, step, p).wait_recv()
                    first, count = carried(step, way)[p]
                    if step == 0 and p == 0:
                        first, count = 0, CUT
                    if step + 2 < far:
                        hop(block, way, step + 1, p).start()
                    elif step + 2 == far:
                        for q, (start, some) in enumerate(last_pieces(way)):
                            if first < start + some <= first + count:
                                hop(block, way, step + 1, q).start()
                    cross(block, first, count)

        def drain(sem, count):
            some = gathered.at[pl.ds(0, count), :]
            pltpu.make_async_copy(some, some, sem).wait()

        drain(d2d_recv, rings * rows)
        drain(ici_send, (rings - 1) * rows - 2 * EARLY)
        drain(d2d_send, rings * rows)
        pltpu.make_async_copy(others, others, peak_send).wait()
        if EARLY:
            pltpu.make_async_copy(early, early, early_send).wait()

    out_shape = (pltpu.VMEM((n * rows, total), jnp.bfloat16),) + tuple(
        pltpu.VMEM((1, w), jnp.float32) for w in widths
    )
    return pl.pallas_call(
        kernel,
        name="update_gather",
        out_shape=out_shape,
        in_specs=[pl.BlockSpec(memory_space=pltpu.HBM)] * 10,
        out_specs=(pl.BlockSpec(memory_space=pltpu.VMEM),) * 4,
        scratch_shapes=[
            pltpu.VMEM((rows, 3 * total), jnp.float32),
            pltpu.VMEM((1, rows), jnp.float32),
            pltpu.VMEM((rows, total), jnp.float32),
            pltpu.VMEM((n, 1, total), jnp.float32),
            pltpu.VMEM((2, max(EARLY, 8), total), jnp.float32),
            pltpu.SemaphoreType.DMA((LOADS,)),
            pltpu.SemaphoreType.DMA((9,)),
            pltpu.SemaphoreType.DMA((slots,)),
        ],
        compiler_params=pltpu.CompilerParams(
            collective_id=0, has_side_effects=True, vmem_limit_bytes=40 * 1024 * 1024
        ),
    )


def put_out(gathered, *refs):
    scales, outs, sems = refs[:3], refs[3:9], refs[9]
    rows, at, copies = gathered.shape[0], 0, []
    for t in range(3):
        width = outs[t].shape[1]
        cuts = 4 if t == 0 else 1
        for first in range(0, rows, rows // cuts):
            span = pl.ds(first, rows // cuts)
            pltpu.make_async_copy(
                gathered.at[span, pl.ds(at, width)], outs[t].at[span, :], sems.at[t]
            ).start()
        copies.append(
            pltpu.make_async_copy(gathered.at[:, pl.ds(at, width)], outs[t], sems.at[t])
        )
        at += width
    for t in range(3):
        copies.append(pltpu.make_async_copy(scales[t], outs[3 + t], sems.at[3 + t]))
        copies[-1].start()
    for copy in copies:
        copy.wait()


def body(
    w_query,
    first_query,
    second_query,
    w_key,
    first_key,
    second_key,
    w_value,
    first_value,
    second_value,
    norm_gain,
):
    n = lax.axis_size(AXIS)
    rows = w_query.shape[0]
    widths = (w_query.shape[1], w_key.shape[1], w_value.shape[1])
    ins = (
        w_query,
        first_query,
        second_query,
        w_key,
        first_key,
        second_key,
        w_value,
        first_value,
        second_value,
        norm_gain.reshape(1, rows),
    )
    ins = [pltpu.with_memory_space_constraint(a, pltpu.HBM) for a in ins]
    held = make_kernel(n, rows, widths)(*ins)
    outs = pl.pallas_call(
        put_out,
        name="put_out",
        out_shape=tuple(jax.ShapeDtypeStruct((n * rows, w), jnp.bfloat16) for w in widths)
        + tuple(jax.ShapeDtypeStruct((1, w), jnp.float32) for w in widths),
        in_specs=[pl.BlockSpec(memory_space=pltpu.VMEM)] * 4,
        out_specs=(pl.BlockSpec(memory_space=pltpu.HBM),) * 6,
        scratch_shapes=[pltpu.SemaphoreType.DMA((6,))],
        compiler_params=pltpu.CompilerParams(vmem_limit_bytes=16 * 1024 * 1024),
    )(*[pltpu.with_memory_space_constraint(a, pltpu.VMEM) for a in held])
    return tuple(outs[:3]) + tuple(s.reshape(-1) for s in outs[3:])


def solution(mesh):
    by_row = P(("shift", "shard"), "width")
    in_specs = (by_row,) * 9 + (P(("shift", "shard")),)
    out_specs = (P("shift", "width"),) * 3 + (P(("shift", "width")),) * 3
    return jax.shard_map(body, mesh=mesh, in_specs=in_specs, out_specs=out_specs, check_vma=False)
```

```python
import functools

import jax
import jax.numpy as jnp
from jax import lax
from jax.experimental import pallas as pl
from jax.experimental.pallas import tpu as pltpu
from jax.sharding import PartitionSpec as P

learn_rate = 0.25
hold_rate = 0.8

MESH = pl.DeviceIdType.MESH
AXIS = "shard"
LOADS = 4
STRIP = 16
EARLY = 32
CUT = 64
FAR_CUTS = ((64, 48, 16), (64, 48, 16))
LENT = 24


def make_kernel(n, rows, widths):
    rings = n // 2
    far = rings // 2
    load_rows = rows // LOADS
    starts = [sum(widths[:t]) for t in range(3)]
    total = sum(widths)
    whole = tuple((first, CUT) for first in range(0, rows, CUT))
    assert sum(map(sum, FAR_CUTS)) == rows

    def last_pieces(way, side):
        first, out = way * sum(FAR_CUTS[0]), []
        for i, count in enumerate(FAR_CUTS[way]):
            if LENT and side == 0 and i == 1:
                count -= LENT
            out.append((first, count))
            first += count
        return tuple(out)

    def lent_rows(way):
        return (way * sum(FAR_CUTS[0]) + sum(FAR_CUTS[way]) - LENT, LENT)

    def carried(step, way, side):
        if step == far - 1:
            return last_pieces(way, side)
        if step == 0 and EARLY:
            return ((EARLY, CUT - EARLY),) + whole[1:]
        return whole

    slots, slot_of = 0, {}
    for way in range(2):
        for step in range(far):
            for p in range(len(carried(step, way, 0))):
                slot_of[way, step, p] = slots
                slots += 1

    def kernel(*refs):
        ins = refs[:10]
        gathered, scales = refs[10], refs[11:14]
        land, gains, fresh, peaks, early = refs[14:19]
        load_sem, one_sem, ici_recv = refs[19:]
        gain_sem, peak_send, peak_recv, ici_send, d2d_send, d2d_recv, early_send = (
            one_sem.at[i] for i in range(7)
        )
        lent_recv = [one_sem.at[9 + way] for way in range(2)]
        lent_cross = [one_sem.at[11 + way] for way in range(2)]

        me = lax.axis_index(AXIS)
        z, core = me // 2, me % 2
        partner = {AXIS: z * 2 + (1 - core)}
        ahead = (lax.rem(z + 1, rings), lax.rem(z + rings - 1, rings))

        barrier = pltpu.get_barrier_semaphore()
        for off in range(1, n):
            pl.semaphore_signal(
                barrier, inc=1, device_id={AXIS: lax.rem(me + off, n)}, device_id_type=MESH
            )

        gain_copy = pltpu.make_async_copy(ins[9], gains, gain_sem)
        gain_copy.start()
        place, at = [], 0
        for t in range(3):
            for _ in range(3):
                place.append((at, widths[t]))
                at += widths[t]
        for part in range(LOADS):
            span = pl.ds(part * load_rows, load_rows)
            for a, (first, width) in enumerate(place):
                pltpu.make_async_copy(
                    ins[a].at[span, :],
                    land.at[span, pl.ds(first, width)],
                    load_sem.at[part],
                ).start()

        gain_copy.wait()
        tall = jnp.transpose(jnp.broadcast_to(gains[...], (128, rows)))
        tops = [jnp.zeros((8, w), jnp.float32) for w in widths]
        for part in range(LOADS):
            span = pl.ds(part * load_rows, load_rows)
            pltpu.make_async_copy(land.at[span, :], land.at[span, :], load_sem.at[part]).wait()
            for r in range(part * load_rows, (part + 1) * load_rows, 8):
                for t in range(3):
                    w, first, second = (
                        land[r : r + 8, place[3 * t + k][0] : place[3 * t + k][0] + widths[t]]
                        for k in range(3)
                    )
                    hold = hold_rate * first + second
                    latest = w - learn_rate * hold
                    gain = jnp.concatenate([tall[r : r + 8, :]] * (widths[t] // 128), axis=1)
                    gained = latest * gain
                    fresh[r : r + 8, starts[t] : starts[t] + widths[t]] = gained
                    tops[t] = jnp.maximum(tops[t], jnp.abs(gained))
        for t in range(3):
            peaks[me, :, starts[t] : starts[t] + widths[t]] = jnp.max(tops[t], axis=0, keepdims=True)

        pl.semaphore_wait(barrier, n - 1)

        for off in sorted(range(1, n), key=lambda off: -min(off, n - off)):
            pltpu.make_async_remote_copy(
                src_ref=peaks.at[me],
                dst_ref=peaks.at[me],
                send_sem=peak_send,
                recv_sem=peak_recv,
                device_id={AXIS: lax.rem(me + off, n)},
                device_id_type=MESH,
            ).start()

        def early_copy(way):
            return pltpu.make_async_remote_copy(
                src_ref=fresh.at[pl.ds(0, EARLY), :],
                dst_ref=early.at[way],
                send_sem=early_send,
                recv_sem=one_sem.at[7 + way],
                device_id={AXIS: ahead[way] * 2 + core},
                device_id_type=MESH,
            )

        if EARLY:
            for way in range(2):
                early_copy(way).start()

        others = peaks.at[pl.ds(0, n - 1)]
        pltpu.make_async_copy(others, others, peak_recv).wait()
        top = jnp.max(peaks[...], axis=0)
        inv = 1.0 / top

        def block_at(distance, way):
            if distance == 0:
                return z
            return lax.rem(z + rings - distance if way == 0 else z + distance, rings)

        def me_rows(block, side=core):
            return pl.multiple_of((block * 2 + side) * rows, STRIP)

        def rows_of(block, first, count, side=core):
            return gathered.at[pl.ds(me_rows(block, side) + first, count), :]

        def carry(block, way, first, count, recv_sem, side=core, to=core):
            return pltpu.make_async_remote_copy(
                src_ref=rows_of(block, first, count, side),
                dst_ref=rows_of(block, first, count, side),
                send_sem=ici_send,
                recv_sem=recv_sem,
                device_id={AXIS: ahead[way] * 2 + to},
                device_id_type=MESH,
            )

        def hop(block, way, step, p, side=0):
            first, count = carried(step, way, side)[p]
            return carry(block, way, first, count, ici_recv.at[slot_of[way, step, p]])

        def across(block, first, count, side=core, recv_sem=d2d_recv):
            return pltpu.make_async_remote_copy(
                src_ref=rows_of(block, first, count, side),
                dst_ref=rows_of(block, first, count, side),
                send_sem=d2d_send,
                recv_sem=recv_sem,
                device_id=partner,
                device_id_type=MESH,
            )

        def cross(block, first, count):
            across(block, first, count).start()

        def each_side(run):
            for side in range(2):
                pl.when(core == side)(functools.partial(run, side))

        def settle(source, base, first, count):
            for r in range(0, count, STRIP):
                row = pl.multiple_of(base + first + r, STRIP)
                gathered[pl.ds(row, STRIP), :] = (source(r) * inv).astype(jnp.bfloat16)

        if EARLY:
            settle(lambda r: fresh[r : r + STRIP, :], me_rows(z), 0, EARLY)
        settle(lambda r: fresh[EARLY + r : EARLY + r + STRIP, :], me_rows(z), EARLY, rows - EARLY)
        for p in range(len(whole)):
            for way in range(2):
                hop(z, way, 0, p).start()
        for first, count in whole:
            cross(z, first, count)
        for t in range(3):
            scales[t][...] = top[:, starts[t] : starts[t] + widths[t]]

        if EARLY:
            for way in range(2):
                early_copy(way).wait_recv()
                settle(lambda r: early[way, r : r + STRIP, :], me_rows(block_at(1, way)), 0, EARLY)

        def last_sent(way, p):
            first, count = whole[p]
            return [
                q
                for q, (start, some) in enumerate(last_pieces(way, 1))
                if first < start + some <= first + count
            ]

        def holds_lent(way, p):
            first, count = whole[p]
            start, some = lent_rows(way)
            return LENT and first <= start and start + some <= first + count

        def onward(block, way, step, p, side):
            for q in last_sent(way, p):
                hop(block, way, step + 1, q, side).start()
            first, count = whole[p]
            if side == 0 and holds_lent(way, p):
                across(block, first, count, recv_sem=lent_cross[way]).start()
            else:
                cross(block, first, count)

        def lend(block, way, p):
            first, count = whole[p]
            across(block, first, count, side=0, recv_sem=lent_cross[way]).wait_recv()
            start, some = lent_rows(way)
            for to in range(2):
                carry(block, way, start, some, lent_recv[way], side=0, to=to).start()

        def arrive(block, way, step, p, side):
            hop(block, way, step, p, side).wait_recv()
            cross(block, *carried(step, way, side)[p])

        def lent_arrive(block, way):
            start, some = lent_rows(way)
            carry(block, way, start, some, lent_recv[way], side=0, to=1).wait_recv()

        for step in range(far):
            for p in range(len(carried(step, 0, 0))):
                for way in range(2):
                    block = block_at(step + 1, way)
                    if step == far - 1:
                        each_side(functools.partial(arrive, block, way, step, p))
                        continue
                    hop(block, way, step, p).wait_recv()
                    if step == far - 2:
                        each_side(functools.partial(onward, block, way, step, p))
                        continue
                    hop(block, way, step + 1, p).start()
                    cross(block, *((0, CUT) if step == 0 and p == 0 else carried(step, way, 0)[p]))
                for way in range(2):
                    if step == far - 2 and holds_lent(way, p):
                        pl.when(core == 1)(
                            functools.partial(lend, block_at(step + 1, way), way, p)
                        )
                    if LENT and step == far - 1 and p == len(carried(step, way, 0)) - 1:
                        lent_arrive(block_at(step + 1, way), way)

        def drain(sem, count):
            some = gathered.at[pl.ds(0, count), :]
            pltpu.make_async_copy(some, some, sem).wait()

        def finish(side):
            lent = 2 * LENT
            drain(d2d_recv, rings * rows - (lent + 2 * CUT if side == 1 and LENT else 0))
            drain(ici_send, (rings - 1) * rows - 2 * EARLY + (2 * lent if side == 1 else -lent))
            drain(d2d_send, rings * rows - (lent if side == 0 else 0))

        each_side(finish)
        pltpu.make_async_copy(others, others, peak_send).wait()
        if EARLY:
            pltpu.make_async_copy(early, early, early_send).wait()

    out_shape = (pltpu.VMEM((n * rows, total), jnp.bfloat16),) + tuple(
        pltpu.VMEM((1, w), jnp.float32) for w in widths
    )
    return pl.pallas_call(
        kernel,
        name="update_gather",
        out_shape=out_shape,
        in_specs=[pl.BlockSpec(memory_space=pltpu.HBM)] * 10,
        out_specs=(pl.BlockSpec(memory_space=pltpu.VMEM),) * 4,
        scratch_shapes=[
            pltpu.VMEM((rows, 3 * total), jnp.float32),
            pltpu.VMEM((1, rows), jnp.float32),
            pltpu.VMEM((rows, total), jnp.float32),
            pltpu.VMEM((n, 1, total), jnp.float32),
            pltpu.VMEM((2, max(EARLY, 8), total), jnp.float32),
            pltpu.SemaphoreType.DMA((LOADS,)),
            pltpu.SemaphoreType.DMA((13,)),
            pltpu.SemaphoreType.DMA((slots,)),
        ],
        compiler_params=pltpu.CompilerParams(
            collective_id=0, has_side_effects=True, vmem_limit_bytes=40 * 1024 * 1024
        ),
    )


def put_out(gathered, *refs):
    scales, outs, sems = refs[:3], refs[3:9], refs[9]
    rows, at, copies = gathered.shape[0], 0, []
    for t in range(3):
        width = outs[t].shape[1]
        cuts = 4 if t == 0 else 1
        for first in range(0, rows, rows // cuts):
            span = pl.ds(first, rows // cuts)
            pltpu.make_async_copy(
                gathered.at[span, pl.ds(at, width)], outs[t].at[span, :], sems.at[t]
            ).start()
        copies.append(
            pltpu.make_async_copy(gathered.at[:, pl.ds(at, width)], outs[t], sems.at[t])
        )
        at += width
    for t in range(3):
        copies.append(pltpu.make_async_copy(scales[t], outs[3 + t], sems.at[3 + t]))
        copies[-1].start()
    for copy in copies:
        copy.wait()


def body(
    w_query,
    first_query,
    second_query,
    w_key,
    first_key,
    second_key,
    w_value,
    first_value,
    second_value,
    norm_gain,
):
    n = lax.axis_size(AXIS)
    rows = w_query.shape[0]
    widths = (w_query.shape[1], w_key.shape[1], w_value.shape[1])
    ins = (
        w_query,
        first_query,
        second_query,
        w_key,
        first_key,
        second_key,
        w_value,
        first_value,
        second_value,
        norm_gain.reshape(1, rows),
    )
    ins = [pltpu.with_memory_space_constraint(a, pltpu.HBM) for a in ins]
    held = make_kernel(n, rows, widths)(*ins)
    outs = pl.pallas_call(
        put_out,
        name="put_out",
        out_shape=tuple(jax.ShapeDtypeStruct((n * rows, w), jnp.bfloat16) for w in widths)
        + tuple(jax.ShapeDtypeStruct((1, w), jnp.float32) for w in widths),
        in_specs=[pl.BlockSpec(memory_space=pltpu.VMEM)] * 4,
        out_specs=(pl.BlockSpec(memory_space=pltpu.HBM),) * 6,
        scratch_shapes=[pltpu.SemaphoreType.DMA((6,))],
        compiler_params=pltpu.CompilerParams(vmem_limit_bytes=16 * 1024 * 1024),
    )(*[pltpu.with_memory_space_constraint(a, pltpu.VMEM) for a in held])
    return tuple(outs[:3]) + tuple(s.reshape(-1) for s in outs[3:])


def solution(mesh):
    by_row = P(("shift", "shard"), "width")
    in_specs = (by_row,) * 9 + (P(("shift", "shard")),)
    out_specs = (P("shift", "width"),) * 3 + (P(("shift", "width")),) * 3
    return jax.shard_map(body, mesh=mesh, in_specs=in_specs, out_specs=out_specs, check_vma=False)
```

```python
import functools

import jax
import jax.numpy as jnp
from jax import lax
from jax.experimental import pallas as pl
from jax.experimental.pallas import tpu as pltpu
from jax.sharding import PartitionSpec as P

learn_rate = 0.25
hold_rate = 0.8

MESH = pl.DeviceIdType.MESH
AXIS = "shard"
LOADS = 4
STRIP = 16
EARLY = 32
CUT = 64
FAR_CUTS = ((64, 48, 16), (64, 48, 16))
LENT = 24


def make_kernel(n, rows, widths):
    rings = n // 2
    far = rings // 2
    load_rows = rows // LOADS
    starts = [sum(widths[:t]) for t in range(3)]
    total = sum(widths)
    whole = tuple((first, CUT) for first in range(0, rows, CUT))
    assert sum(map(sum, FAR_CUTS)) == rows

    def last_pieces(way, side):
        first, out = way * sum(FAR_CUTS[0]), []
        for i, count in enumerate(FAR_CUTS[way]):
            if LENT and side == 0 and i == 1:
                count -= LENT
            out.append((first, count))
            first += count
        return tuple(out)

    def lent_rows(way):
        return (way * sum(FAR_CUTS[0]) + sum(FAR_CUTS[way]) - LENT, LENT)

    def carried(step, way, side):
        if step == far - 1:
            return last_pieces(way, side)
        if step == 0 and EARLY:
            return ((EARLY, CUT - EARLY),) + whole[1:]
        return whole

    slots, slot_of = 0, {}
    for way in range(2):
        for step in range(far):
            for p in range(len(carried(step, way, 0))):
                slot_of[way, step, p] = slots
                slots += 1

    def kernel(*refs):
        ins = refs[:10]
        gathered, scales = refs[10], refs[11:14]
        land, gains, fresh, peaks, early = refs[14:19]
        load_sem, one_sem, ici_recv = refs[19:]
        gain_sem, peak_send, peak_recv, ici_send, d2d_send, d2d_recv, early_send = (
            one_sem.at[i] for i in range(7)
        )
        lent_recv = [one_sem.at[9 + way] for way in range(2)]
        lent_cross = [one_sem.at[11 + way] for way in range(2)]

        me = lax.axis_index(AXIS)
        z, core = me // 2, me % 2
        partner = {AXIS: z * 2 + (1 - core)}
        ahead = (lax.rem(z + 1, rings), lax.rem(z + rings - 1, rings))

        barrier = pltpu.get_barrier_semaphore()
        for off in range(1, n):
            pl.semaphore_signal(
                barrier, inc=1, device_id={AXIS: lax.rem(me + off, n)}, device_id_type=MESH
            )

        gain_copy = pltpu.make_async_copy(ins[9], gains, gain_sem)
        gain_copy.start()
        place, at = [], 0
        for t in range(3):
            for _ in range(3):
                place.append((at, widths[t]))
                at += widths[t]
        for part in range(LOADS):
            span = pl.ds(part * load_rows, load_rows)
            for a, (first, width) in enumerate(place):
                pltpu.make_async_copy(
                    ins[a].at[span, :],
                    land.at[span, pl.ds(first, width)],
                    load_sem.at[part],
                ).start()

        gain_copy.wait()
        tall = jnp.transpose(jnp.broadcast_to(gains[...], (128, rows)))
        tops = [jnp.zeros((8, w), jnp.float32) for w in widths]
        for part in range(LOADS):
            span = pl.ds(part * load_rows, load_rows)
            pltpu.make_async_copy(land.at[span, :], land.at[span, :], load_sem.at[part]).wait()
            for r in range(part * load_rows, (part + 1) * load_rows, 8):
                for t in range(3):
                    w, first, second = (
                        land[r : r + 8, place[3 * t + k][0] : place[3 * t + k][0] + widths[t]]
                        for k in range(3)
                    )
                    hold = hold_rate * first + second
                    latest = w - learn_rate * hold
                    gain = jnp.concatenate([tall[r : r + 8, :]] * (widths[t] // 128), axis=1)
                    gained = latest * gain
                    fresh[r : r + 8, starts[t] : starts[t] + widths[t]] = gained
                    tops[t] = jnp.maximum(tops[t], jnp.abs(gained))
        for t in range(3):
            peaks[me, :, starts[t] : starts[t] + widths[t]] = jnp.max(tops[t], axis=0, keepdims=True)

        pl.semaphore_wait(barrier, n - 1)

        for off in sorted(range(1, n), key=lambda off: -min(off, n - off)):
            pltpu.make_async_remote_copy(
                src_ref=peaks.at[me],
                dst_ref=peaks.at[me],
                send_sem=peak_send,
                recv_sem=peak_recv,
                device_id={AXIS: lax.rem(me + off, n)},
                device_id_type=MESH,
            ).start()

        def early_copy(way, first=0, count=EARLY):
            return pltpu.make_async_remote_copy(
                src_ref=fresh.at[pl.ds(first, count), :],
                dst_ref=early.at[way, pl.ds(first, count), :],
                send_sem=early_send,
                recv_sem=one_sem.at[7 + way],
                device_id={AXIS: ahead[way] * 2 + core},
                device_id_type=MESH,
            )

        if EARLY:
            for first in range(0, EARLY, STRIP // 2):
                for way in range(2):
                    early_copy(way, first, STRIP // 2).start()

        others = peaks.at[pl.ds(0, n - 1)]
        pltpu.make_async_copy(others, others, peak_recv).wait()
        top = jnp.max(peaks[...], axis=0)
        inv = 1.0 / top

        def block_at(distance, way):
            if distance == 0:
                return z
            return lax.rem(z + rings - distance if way == 0 else z + distance, rings)

        def me_rows(block, side=core):
            return pl.multiple_of((block * 2 + side) * rows, STRIP)

        def rows_of(block, first, count, side=core):
            return gathered.at[pl.ds(me_rows(block, side) + first, count), :]

        def carry(block, way, first, count, recv_sem, side=core, to=core):
            return pltpu.make_async_remote_copy(
                src_ref=rows_of(block, first, count, side),
                dst_ref=rows_of(block, first, count, side),
                send_sem=ici_send,
                recv_sem=recv_sem,
                device_id={AXIS: ahead[way] * 2 + to},
                device_id_type=MESH,
            )

        def hop(block, way, step, p, side=0):
            first, count = carried(step, way, side)[p]
            return carry(block, way, first, count, ici_recv.at[slot_of[way, step, p]])

        def across(block, first, count, side=core, recv_sem=d2d_recv):
            return pltpu.make_async_remote_copy(
                src_ref=rows_of(block, first, count, side),
                dst_ref=rows_of(block, first, count, side),
                send_sem=d2d_send,
                recv_sem=recv_sem,
                device_id=partner,
                device_id_type=MESH,
            )

        def cross(block, first, count):
            across(block, first, count).start()

        def each_side(run):
            for side in range(2):
                pl.when(core == side)(functools.partial(run, side))

        def settle(source, base, first, count):
            for r in range(0, count, STRIP):
                row = pl.multiple_of(base + first + r, STRIP)
                gathered[pl.ds(row, STRIP), :] = (source(r) * inv).astype(jnp.bfloat16)

        if EARLY:
            settle(lambda r: fresh[r : r + STRIP, :], me_rows(z), 0, EARLY)
        settle(lambda r: fresh[EARLY + r : EARLY + r + STRIP, :], me_rows(z), EARLY, rows - EARLY)
        for p in range(len(whole)):
            for way in range(2):
                hop(z, way, 0, p).start()
        for first, count in whole:
            cross(z, first, count)
        for t in range(3):
            scales[t][...] = top[:, starts[t] : starts[t] + widths[t]]

        if EARLY:
            for way in range(2):
                early_copy(way).wait_recv()
                settle(lambda r: early[way, r : r + STRIP, :], me_rows(block_at(1, way)), 0, EARLY)

        def last_sent(way, p):
            first, count = whole[p]
            return [
                q
                for q, (start, some) in enumerate(last_pieces(way, 1))
                if first < start + some <= first + count
            ]

        def holds_lent(way, p):
            first, count = whole[p]
            start, some = lent_rows(way)
            return LENT and first <= start and start + some <= first + count

        def onward(block, way, step, p, side):
            for q in last_sent(way, p):
                hop(block, way, step + 1, q, side).start()
            first, count = whole[p]
            if side == 0 and holds_lent(way, p):
                across(block, first, count, recv_sem=lent_cross[way]).start()
            else:
                cross(block, first, count)

        def lend(block, way, p):
            first, count = whole[p]
            across(block, first, count, side=0, recv_sem=lent_cross[way]).wait_recv()
            start, some = lent_rows(way)
            for to in range(2):
                carry(block, way, start, some, lent_recv[way], side=0, to=to).start()

        def arrive(block, way, step, p, side):
            hop(block, way, step, p, side).wait_recv()
            cross(block, *carried(step, way, side)[p])

        def lent_arrive(block, way):
            start, some = lent_rows(way)
            carry(block, way, start, some, lent_recv[way], side=0, to=1).wait_recv()

        for step in range(far):
            for p in range(len(carried(step, 0, 0))):
                for way in range(2):
                    block = block_at(step + 1, way)
                    if step == far - 1:
                        each_side(functools.partial(arrive, block, way, step, p))
                        continue
                    hop(block, way, step, p).wait_recv()
                    if step == far - 2:
                        each_side(functools.partial(onward, block, way, step, p))
                        continue
                    hop(block, way, step + 1, p).start()
                    cross(block, *((0, CUT) if step == 0 and p == 0 else carried(step, way, 0)[p]))
                for way in range(2):
                    if step == far - 2 and holds_lent(way, p):
                        pl.when(core == 1)(
                            functools.partial(lend, block_at(step + 1, way), way, p)
                        )
                    if LENT and step == far - 1 and p == len(carried(step, way, 0)) - 1:
                        lent_arrive(block_at(step + 1, way), way)

        def drain(sem, count):
            some = gathered.at[pl.ds(0, count), :]
            pltpu.make_async_copy(some, some, sem).wait()

        def finish(side):
            lent = 2 * LENT
            drain(d2d_recv, rings * rows - (lent + 2 * CUT if side == 1 and LENT else 0))
            drain(ici_send, (rings - 1) * rows - 2 * EARLY + (2 * lent if side == 1 else -lent))
            drain(d2d_send, rings * rows - (lent if side == 0 else 0))

        each_side(finish)
        pltpu.make_async_copy(others, others, peak_send).wait()
        if EARLY:
            pltpu.make_async_copy(early, early, early_send).wait()

    out_shape = (pltpu.VMEM((n * rows, total), jnp.bfloat16),) + tuple(
        pltpu.VMEM((1, w), jnp.float32) for w in widths
    )
    return pl.pallas_call(
        kernel,
        name="update_gather",
        out_shape=out_shape,
        in_specs=[pl.BlockSpec(memory_space=pltpu.HBM)] * 10,
        out_specs=(pl.BlockSpec(memory_space=pltpu.VMEM),) * 4,
        scratch_shapes=[
            pltpu.VMEM((rows, 3 * total), jnp.float32),
            pltpu.VMEM((1, rows), jnp.float32),
            pltpu.VMEM((rows, total), jnp.float32),
            pltpu.VMEM((n, 1, total), jnp.float32),
            pltpu.VMEM((2, max(EARLY, 8), total), jnp.float32),
            pltpu.SemaphoreType.DMA((LOADS,)),
            pltpu.SemaphoreType.DMA((13,)),
            pltpu.SemaphoreType.DMA((slots,)),
        ],
        compiler_params=pltpu.CompilerParams(
            collective_id=0, has_side_effects=True, vmem_limit_bytes=40 * 1024 * 1024
        ),
    )


def put_out(gathered, *refs):
    scales, outs, sems = refs[:3], refs[3:9], refs[9]
    rows, at, copies = gathered.shape[0], 0, []
    for t in range(3):
        width = outs[t].shape[1]
        cuts = 4 if t == 0 else 1
        for first in range(0, rows, rows // cuts):
            span = pl.ds(first, rows // cuts)
            pltpu.make_async_copy(
                gathered.at[span, pl.ds(at, width)], outs[t].at[span, :], sems.at[t]
            ).start()
        copies.append(
            pltpu.make_async_copy(gathered.at[:, pl.ds(at, width)], outs[t], sems.at[t])
        )
        at += width
    for t in range(3):
        copies.append(pltpu.make_async_copy(scales[t], outs[3 + t], sems.at[3 + t]))
        copies[-1].start()
    for copy in copies:
        copy.wait()


def body(
    w_query,
    first_query,
    second_query,
    w_key,
    first_key,
    second_key,
    w_value,
    first_value,
    second_value,
    norm_gain,
):
    n = lax.axis_size(AXIS)
    rows = w_query.shape[0]
    widths = (w_query.shape[1], w_key.shape[1], w_value.shape[1])
    ins = (
        w_query,
        first_query,
        second_query,
        w_key,
        first_key,
        second_key,
        w_value,
        first_value,
        second_value,
        norm_gain.reshape(1, rows),
    )
    ins = [pltpu.with_memory_space_constraint(a, pltpu.HBM) for a in ins]
    held = make_kernel(n, rows, widths)(*ins)
    outs = pl.pallas_call(
        put_out,
        name="put_out",
        out_shape=tuple(jax.ShapeDtypeStruct((n * rows, w), jnp.bfloat16) for w in widths)
        + tuple(jax.ShapeDtypeStruct((1, w), jnp.float32) for w in widths),
        in_specs=[pl.BlockSpec(memory_space=pltpu.VMEM)] * 4,
        out_specs=(pl.BlockSpec(memory_space=pltpu.HBM),) * 6,
        scratch_shapes=[pltpu.SemaphoreType.DMA((6,))],
        compiler_params=pltpu.CompilerParams(vmem_limit_bytes=16 * 1024 * 1024),
    )(*[pltpu.with_memory_space_constraint(a, pltpu.VMEM) for a in held])
    return tuple(outs[:3]) + tuple(s.reshape(-1) for s in outs[3:])


def solution(mesh):
    by_row = P(("shift", "shard"), "width")
    in_specs = (by_row,) * 9 + (P(("shift", "shard")),)
    out_specs = (P("shift", "width"),) * 3 + (P(("shift", "width")),) * 3
    return jax.shard_map(body, mesh=mesh, in_specs=in_specs, out_specs=out_specs, check_vma=False)
```
